32 devices in a mesh: dom: 8 (over z, y), cls: 4 (over x, core).
Axes of the slice: x: 2, y: 2, z: 4, core: 2. Of those that a mesh axis runs over, the one named last changes fastest.
Arguments:
- images: bfloat16 [4096, 2, 16384], P(('dom', 'cls')), may hold values from -6 to 6
- slices: bfloat16 [32, 4, 2, 16384], P(('dom', 'cls')), may hold values from -6 to 6
- classes: int32 [4096], P(('dom', 'cls')), may hold values from 0 to 31, as said below
- rotations: int32 [4096], P(('dom', 'cls')), may hold values from 0 to 3
- defocus: int32 [4096], P(('dom', 'cls')), may hold values from 8000 to 29999
- groups: int32 [4096], P(('dom', 'cls')), may hold values from 0 to 255, as said below
Outputs:
- sigma: float32 [256, 64], P(('dom', 'cls'))
The draws below stay inside these ranges and needn't reach their ends.
Inputs may be any that keep to these rules, and one draw needn't show every extreme that they name: Class c is owned by device c // 1 of dom+cls. In the rows of one device, at most 8 particles have classes of one owner; in every draw one owner gets exactly 8 from the rows of every device. `groups`: group g is owned by device g // 8 of dom+cls. Every group holds at least 8 particles.
All inputs are finite; a program needn't handle non-finite values.
Results may differ from the reference program's by a relative error of at most 0.0003.
Values may be sent and summed in bfloat16 or wider, within the bound.
A program may use at most 192 MiB of HBM per device.

```python
import math
import jax
import jax.numpy as jnp
from jax import lax

SIDE = 128
PIX = 16384
SHELLS = 64
ROT = 4
CLS_DEV = 1
CLASSES = 32
P_DEV = 128
PARTICLES = 4096
CAP = 8
GROUPS_DEV = 8
GROUPS = 256


def draw_classes(key, part):
    owner_count = CLASSES // CLS_DEV
    block_count = PARTICLES // P_DEV
    slot_count = owner_count * CAP
    key_popular, key_bias, key_blocks = jax.random.split(jax.random.fold_in(key, 11), 3)
    popular = jax.random.randint(key_popular, (), 0, owner_count)
    owner_bias = jax.random.randint(key_bias, (owner_count,), 0, 4096)

    def one_block(block_index):
        block_key = jax.random.fold_in(key_blocks, block_index)
        key_noise, key_order, key_within = jax.random.split(block_key, 3)
        noise = jax.random.randint(key_noise, (owner_count, CAP), 0, 4096)
        owner_ids = jnp.broadcast_to(jnp.arange(owner_count, dtype=jnp.int32)[:, None], (owner_count, CAP))
        scores = owner_bias[:, None] + noise + jnp.where(owner_ids == popular, 16384, 0)
        distinct = scores.reshape(-1) * slot_count + jnp.arange(slot_count, dtype=jnp.int32)
        chosen_values, picked = lax.top_k(distinct, P_DEV)
        owner_of = picked.astype(jnp.int32) // CAP
        shuffle = jax.random.permutation(key_order, P_DEV)
        owner_of = owner_of[shuffle]
        within = jax.random.randint(key_within, (P_DEV,), 0, CLS_DEV)
        return owner_of * CLS_DEV + within
    return jax.vmap(one_block)(jnp.arange(block_count, dtype=jnp.int32)).reshape(-1).astype(jnp.int32)


def draw_groups(key, part):
    block_count = PARTICLES // P_DEV
    half_rows = P_DEV // 2
    key_random, key_order = jax.random.split(jax.random.fold_in(key, 23), 2)
    device_ids = jnp.arange(block_count, dtype=jnp.int32)[:, None]
    row_ids = jnp.arange(P_DEV, dtype=jnp.int32)[None, :]
    far_owner = (device_ids + block_count // 2) % block_count
    far_group = far_owner * GROUPS_DEV + row_ids % GROUPS_DEV
    random_group = jax.random.randint(key_random, (block_count, P_DEV), 0, GROUPS)
    base = jnp.where(row_ids < half_rows, far_group, random_group)
    order_keys = jax.random.split(key_order, block_count)
    orders = jax.vmap(lambda one_key: jax.random.permutation(one_key, P_DEV))(order_keys)
    mixed = jnp.take_along_axis(base, orders.astype(jnp.int32), axis=1)
    return mixed.reshape(-1).astype(jnp.int32)


def set_ends(array, key, least, high):
    index_at = [jax.random.randint(jax.random.fold_in(key, axis), (), 0, length) for axis, length in enumerate(array.shape)]
    main_axis = array.shape.index(max(array.shape))
    neighbour = index_at[:main_axis] + [(index_at[main_axis] + 1) % array.shape[main_axis]] + index_at[main_axis + 1:]
    return array.at[tuple(index_at)].set(least).at[tuple(neighbour)].set(high)


def shard_levels(rng, extent, pieces, low, top_value):
    loudness, own = 1.0, jax.random.fold_in(rng, 6)
    for dim, shards_of in pieces:
        heights = jnp.exp(jax.random.uniform(jax.random.fold_in(own, dim), (shards_of,), jnp.float32, low / len(pieces), top_value / len(pieces)))
        loudness = loudness * jnp.repeat(heights, extent[dim] // shards_of).reshape([-1 if axis == dim else 1 for axis in range(len(extent))])
    return loudness


def gaussian(stream_key, dims, scale, bound, shards=(), kind=jnp.bfloat16):
    drawn = scale * jax.random.normal(stream_key, dims, jnp.float32)
    if shards:
        drawn = drawn * shard_levels(stream_key, dims, shards, -0.22, 0.18)
    return jnp.clip(drawn, -bound, bound).astype(kind)


def setup_inputs(seed: int = 0) -> dict:
    key_list = jax.random.split(jax.random.key(seed), 7)
    return {
        "images": gaussian(key_list[0], (PARTICLES, 2, PIX), 1.0, 6.0, ((0, 32),)),
        "slices": gaussian(key_list[1], (CLASSES, ROT, 2, PIX), 1.0, 6.0, ((0, 32),)),
        "classes": draw_classes(jax.random.fold_in(key_list[6], 71), 0),
        "rotations": set_ends(jax.random.randint(key_list[3], (PARTICLES,), 0, ROT), jax.random.fold_in(key_list[3], 1), 0, ROT - 1).astype(jnp.int32),
        "defocus": set_ends(jax.random.randint(key_list[4], (PARTICLES,), 8000, 30000), jax.random.fold_in(key_list[4], 1), 8000, 29999).astype(jnp.int32),
        "groups": draw_groups(jax.random.fold_in(key_list[6], 71), 0),
    }


PIXEL_SIZE = 1.5
WAVELENGTH = 0.0197
SPHERICAL = 27000000.0
AMPLITUDE = 0.1

def frequency_grid(side_cells):
    offsets = jnp.arange(side_cells, dtype=jnp.int32)
    signed = jnp.where(offsets < side_cells // 2, offsets, offsets - side_cells)
    return (signed[:, None] * signed[:, None] + signed[None, :] * signed[None, :]).reshape(-1).astype(jnp.int32)

def shell_matrix(radius_sq, shell_count):
    shell_ids = jnp.arange(shell_count, dtype=jnp.int32)
    lower = shell_ids * shell_ids
    upper = (shell_ids + 1) * (shell_ids + 1)
    in_shell = (lower[None, :] <= radius_sq[:, None]) & (radius_sq[:, None] < upper[None, :])
    return in_shell.astype(jnp.float32)

def contrast(defocus, radius_sq, side_cells):
    spatial = radius_sq.astype(jnp.float32) / jnp.float32((side_cells * PIXEL_SIZE) ** 2)
    depth = defocus.astype(jnp.float32)[:, None]
    phase_shift = math.pi * WAVELENGTH * depth * spatial[None, :] - 0.5 * math.pi * SPHERICAL * WAVELENGTH ** 3 * spatial[None, :] * spatial[None, :]
    return -(math.sqrt(1.0 - AMPLITUDE * AMPLITUDE) * jnp.sin(phase_shift) + AMPLITUDE * jnp.cos(phase_shift))

def power_in_shells(images, fetched, ctf, shell_table):
    difference = images.astype(jnp.float32) - ctf[:, None, :] * fetched.astype(jnp.float32)
    pixel_power = lax.optimization_barrier(jnp.sum(difference * difference, axis=1))
    return jnp.dot(pixel_power, shell_table, precision=lax.Precision.HIGHEST, preferred_element_type=jnp.float32)

def reference(images, slices, classes, rotations, defocus, groups):
    radius_sq = frequency_grid(SIDE)
    shell_table = shell_matrix(radius_sq, SHELLS)
    block_rows = math.gcd(PARTICLES, 512)
    block_count = PARTICLES // block_rows

    def per_block(operands):
        image_rows, class_rows, rotation_rows, defocus_rows = operands
        fetched = slices[class_rows, rotation_rows]
        ctf = contrast(defocus_rows, radius_sq, SIDE)
        return power_in_shells(image_rows, fetched, ctf, shell_table)
    shell_power = lax.map(per_block, (images.reshape(block_count, block_rows, 2, PIX), classes.reshape(block_count, block_rows), rotations.reshape(block_count, block_rows), defocus.reshape(block_count, block_rows))).reshape(PARTICLES, SHELLS)
    group_sums = jax.ops.segment_sum(shell_power, groups, num_segments=GROUPS)
    group_counts = jax.ops.segment_sum(jnp.ones((PARTICLES,), jnp.float32), groups, num_segments=GROUPS)
    pixel_counts = lax.optimization_barrier(jnp.sum(shell_table, axis=0))
    return group_sums / (2.0 * group_counts[:, None] * pixel_counts[None, :])
```

```python
import functools
import math

import jax
import jax.numpy as jnp
import numpy as np
from jax import lax
from jax.experimental import pallas as pl
from jax.experimental.pallas import tpu as pltpu
from jax.sharding import PartitionSpec as P

GROUPS_DEV = 8
PIXEL_SIZE = 1.5
WAVELENGTH = 0.0197
SPHERICAL = 27000000.0
AMPLITUDE = 0.1
MESH = pl.DeviceIdType.MESH
AXES = ("dom", "cls")
ROUTES = (("x", "y", "z"), ("z", "y", "x"), ("z", "x", "y"))
SHARE = (8, 12, 12)


def sine_coefficients(terms):
    nodes = 0.5 * np.cos((np.arange(400) + 0.5) * math.pi / 400)
    nodes = nodes[np.abs(nodes) > 1e-3]
    basis = np.stack([nodes ** (2 * k + 1) for k in range(terms)], 1)
    return np.linalg.lstsq(basis, np.sin(2 * math.pi * nodes), rcond=None)[0]


SINE = [float(v) for v in sine_coefficients(6)]


def gather_kernel(shape, own_ref, out_ref, local_sem, send_sem, recv_sem, pair_send, pair_recv):
    size = dict(x=shape[0], y=shape[1], z=shape[2])
    dom, cls = lax.axis_index("dom"), lax.axis_index("cls")
    here = dict(x=cls // 2, y=dom % size["y"], z=dom // size["y"])
    core = cls % 2
    rows = out_ref.shape[2]
    starts = [0]
    for share in SHARE:
        starts.append(starts[-1] + rows * share // 32)

    def device(at, which):
        return (at["z"] * size["y"] + at["y"], at["x"] * 2 + which)

    def slot(at, which):
        d = device(at, which)
        return d[0] * (size["x"] * 2) + d[1]

    def moved(at, dim, step):
        new = dict(at)
        new[dim] = at[dim] + step
        return new

    ways = []
    for dim in "xyz":
        if size[dim] == 1:
            continue
        if size[dim] == 2:
            other = dict(here)
            other[dim] = 1 - here[dim]
            ways.append((dim, 0, other, None))
        else:
            ways.append((dim, 1, moved(here, dim, 1), here[dim] < size[dim] - 1))
            ways.append((dim, -1, moved(here, dim, -1), here[dim] > 0))

    def when(conds, fn):
        conds = [c for c in conds if c is not None]
        if not conds:
            fn()
        else:
            pl.when(functools.reduce(jnp.logical_and, conds))(fn)

    barrier = pltpu.get_barrier_semaphore()
    partner = device(here, 1 - core)
    pl.semaphore_signal(barrier, inc=1, device_id=partner, device_id_type=MESH)
    for dim, sign, other, ok in ways:

        def greet(other=other):
            pl.semaphore_signal(barrier, inc=1, device_id=device(other, core), device_id_type=MESH)

        when([ok], greet)
    peers = 1
    for dim, sign, other, ok in ways:
        peers = peers + (1 if ok is None else ok.astype(jnp.int32))
    pl.semaphore_wait(barrier, peers)

    mine = slot(here, core)
    local = pltpu.make_async_copy(own_ref, out_ref.at[mine], local_sem)
    local.start()

    def part(ref, index):
        return ref.at[:, pl.ds(starts[index], starts[index + 1] - starts[index]), :]

    def copy(index, source, src_slot, to, way, own):
        src = part(own_ref, index) if own else part(out_ref.at[src_slot], index)
        return pltpu.make_async_remote_copy(
            src_ref=src,
            dst_ref=part(out_ref.at[src_slot], index),
            send_sem=send_sem.at[index, source, way],
            recv_sem=recv_sem.at[index, src_slot],
            device_id=to,
            device_id_type=MESH,
        )

    def pair_copy(index, source, src_slot, own):
        src = part(own_ref, index) if own else part(out_ref.at[src_slot], index)
        return pltpu.make_async_remote_copy(
            src_ref=src,
            dst_ref=part(out_ref.at[src_slot], index),
            send_sem=pair_send.at[index, source],
            recv_sem=pair_recv.at[index, src_slot],
            device_id=partner,
            device_id_type=MESH,
        )

    choices = {}
    for dim in "xyz":
        n = size[dim]
        if n == 1:
            choices[dim] = [(0, here[dim], None, 0)]
        elif n == 2:
            choices[dim] = [(0, here[dim], None, 0), (0, 1 - here[dim], None, 1)]
        else:
            listed = [(0, here[dim], None, 0)]
            for t in range(1, n):
                listed.append((1, here[dim] - t, here[dim] >= t, t))
                listed.append((-1, here[dim] + t, here[dim] + t < n, t))
            choices[dim] = listed
    events = []
    for ix, cx in enumerate(choices["x"]):
        for iy, cy in enumerate(choices["y"]):
            for iz, cz in enumerate(choices["z"]):
                pick = dict(x=cx, y=cy, z=cz)
                depth = cx[3] + cy[3] + cz[3]
                number = (ix * len(choices["y"]) + iy) * len(choices["z"]) + iz
                for index in range(3):
                    events.append((depth, index, number, pick))
    events.sort(key=lambda e: e[:3])
    finish = []
    for depth, index, number, pick in events:
        at = {dim: pick[dim][1] for dim in "xyz"}
        exists = [pick[dim][2] for dim in "xyz"]
        src_slot = slot(at, core)
        order = ROUTES[index]
        last = max([k for k, dim in enumerate(order) if pick[dim][3] > 0], default=-1)
        sends = []
        for number_way, (dim, sign, other, ok) in enumerate(ways):
            k = order.index(dim)
            if k < last:
                continue
            if k == last and (size[dim] == 2 or sign != pick[dim][0]):
                continue
            sends.append((number_way, device(other, core), ok))

        def arrive(index=index, number=number, src_slot=src_slot, depth=depth, sends=sends):
            own = depth == 0
            if not own:
                copy(index, number, src_slot, partner, 0, False).wait_recv()
            for way, to, ok in sends:
                when([ok], copy(index, number, src_slot, to, way, own).start)
            pair_copy(index, number, src_slot, own).start()

        def done(index=index, number=number, src_slot=src_slot, depth=depth, sends=sends, at=at):
            own = depth == 0
            for way, to, ok in sends:
                when([ok], copy(index, number, src_slot, to, way, own).wait_send)
            pair_copy(index, number, src_slot, own).wait_send()
            pair_copy(index, number, slot(at, 1 - core), False).wait_recv()

        when(exists, arrive)
        finish.append((exists, done))
    for exists, done in finish:
        when(exists, done)
    local.wait()


def gather(shape, own):
    devices = 2 * shape[0] * shape[1] * shape[2]
    total = 1
    for n in shape:
        total *= n if n <= 2 else 2 * n - 1
    return pl.pallas_call(
        functools.partial(gather_kernel, shape),
        out_shape=jax.ShapeDtypeStruct((devices,) + own.shape, own.dtype),
        in_specs=[pl.BlockSpec(memory_space=pltpu.VMEM)],
        out_specs=pl.BlockSpec(memory_space=pltpu.VMEM),
        scratch_shapes=[
            pltpu.SemaphoreType.DMA,
            pltpu.SemaphoreType.DMA((3, total, 4)),
            pltpu.SemaphoreType.DMA((3, devices)),
            pltpu.SemaphoreType.DMA((3, total)),
            pltpu.SemaphoreType.DMA((3, devices)),
        ],
        compiler_params=pltpu.CompilerParams(
            collective_id=0, has_side_effects=True, vmem_limit_bytes=32 * 1024 * 1024
        ),
        name="gather_slices",
    )(own)


def power_kernel(
    side, rot_count, index_ref, depth_ref, images_ref, slices_ref, slope_ref, offset_ref, groups_ref, out_ref, power, acc
):
    step = pl.program_id(0)
    count, chunk, lanes = images_ref.shape
    shells = side // 2

    @pl.when(step == 0)
    def _():
        acc[...] = jnp.zeros_like(acc)

    slope = slope_ref[...]
    offset = offset_ref[...]

    def one(i, carry):
        turns = depth_ref[i] * slope + offset
        x = turns - jnp.round(turns)
        y = x * x
        s = jnp.full_like(y, SINE[-1])
        for value in SINE[-2::-1]:
            s = s * y + value
        s = s * x
        d = images_ref[i].astype(jnp.float32) + s * slices_ref[index_ref[i], pl.ds(pl.multiple_of(step * chunk, chunk), chunk), :].astype(jnp.float32)
        power[pl.ds(pl.multiple_of(i * chunk, chunk), chunk), :] = d * d
        return carry

    lax.fori_loop(0, count, one, 0, unroll=4)

    b = lax.broadcasted_iota(jnp.int32, (lanes, shells), 0)
    s = lax.broadcasted_iota(jnp.int32, (lanes, shells), 1)
    fb = jnp.where(b < side // 2, b, b - side)
    total = acc[...]
    for k in range(chunk // 2):
        a = step * (chunk // 2) + k
        fa = jnp.where(a < side // 2, a, a - side)
        r = fa * fa + fb * fb
        table = jnp.where((s * s <= r) & (r < (s + 1) * (s + 1)), 1.0, 0.0).astype(jnp.bfloat16)
        p = power[pl.ds(2 * k, count, stride=chunk), :] + power[pl.ds(2 * k + 1, count, stride=chunk), :]
        high = p.astype(jnp.bfloat16)
        low = (p - high.astype(jnp.float32)).astype(jnp.bfloat16)
        total = total + (
            jnp.dot(high, table, preferred_element_type=jnp.float32)
            + jnp.dot(low, table, preferred_element_type=jnp.float32)
        )
    acc[...] = total

    @pl.when(step == pl.num_programs(0) - 1)
    def _():
        groups = out_ref.shape[0]
        ids = lax.broadcasted_iota(jnp.int32, (groups, count), 0)
        member = jnp.where(ids == groups_ref[...], 1.0, 0.0)
        both = jnp.concatenate([acc[...], jnp.ones((count, out_ref.shape[1] - shells), jnp.float32)], axis=1)
        out_ref[...] = jnp.dot(
            member, both, precision=lax.Precision.HIGHEST, preferred_element_type=jnp.float32
        )


def shell_power(images, slices, index, defocus, groups, group_total):
    count, rows, side = images.shape
    chunk = 32
    offsets = np.arange(side)
    signed = np.where(offsets < side // 2, offsets, offsets - side)
    radius = (signed[:, None] ** 2 + signed[None, :] ** 2).astype(np.float64)
    spatial = np.repeat(radius / (side * PIXEL_SIZE) ** 2, 2, axis=0)
    slope = (0.5 * WAVELENGTH * spatial).astype(np.float32)
    offset = -0.25 * SPHERICAL * WAVELENGTH**3 * spatial**2 + math.asin(AMPLITUDE) / (2 * math.pi)
    offset = (offset - np.round(offset)).astype(np.float32)
    smem = pl.BlockSpec(memory_space=pltpu.SMEM)
    return pl.pallas_call(
        functools.partial(power_kernel, side, 4),
        grid=(rows // chunk,),
        out_shape=jax.ShapeDtypeStruct((group_total, 128), jnp.float32),
        in_specs=[
            smem,
            smem,
            pl.BlockSpec((count, chunk, side), lambda i: (0, i, 0)),
            pl.BlockSpec(memory_space=pltpu.VMEM),
            pl.BlockSpec((chunk, side), lambda i: (i, 0)),
            pl.BlockSpec((chunk, side), lambda i: (i, 0)),
            pl.BlockSpec((1, count), lambda i: (0, 0)),
        ],
        out_specs=pl.BlockSpec((group_total, 128), lambda i: (0, 0)),
        scratch_shapes=[
            pltpu.VMEM((count * chunk, side), jnp.float32),
            pltpu.VMEM((count, side // 2), jnp.float32),
        ],
        compiler_params=pltpu.CompilerParams(vmem_limit_bytes=48 * 1024 * 1024),
        name="shell_power",
    )(index, defocus.astype(jnp.float32), images, slices, jnp.asarray(slope), jnp.asarray(offset), groups.reshape(1, count))


def exchange_kernel(sizes, shells, parts_ref, weight_ref, out_ref, held, send_sem, recv_sem):
    doms, clss = sizes
    n = doms * clss
    me = lax.axis_index("dom") * clss + lax.axis_index("cls")
    barrier = pltpu.get_barrier_semaphore()

    def device(k):
        peer = lax.rem(me + k, n)
        return peer, (peer // clss, lax.rem(peer, clss))

    def greet(k, carry):
        pl.semaphore_signal(barrier, inc=1, device_id=device(k)[1], device_id_type=MESH)
        return carry

    lax.fori_loop(1, n, greet, 0)
    pl.semaphore_wait(barrier, n - 1)

    def copy(k):
        peer, to = device(k)
        return pltpu.make_async_remote_copy(
            src_ref=parts_ref.at[peer],
            dst_ref=held.at[k],
            send_sem=send_sem.at[k],
            recv_sem=recv_sem.at[k],
            device_id=to,
            device_id_type=MESH,
        )

    def send(k, carry):
        copy(k).start()
        return carry

    lax.fori_loop(1, n, send, 0)

    def take(k, total):
        copy(k).wait_recv()
        return total + held[k]

    total = lax.fori_loop(1, n, take, parts_ref[me])

    def sent(k, carry):
        copy(k).wait_send()
        return carry

    lax.fori_loop(1, n, sent, 0)
    counts = total[:, shells : shells + 1]
    out_ref[...] = total[:, :shells] / (2.0 * counts * weight_ref[...])


def exchange(sizes, parts, weight):
    n = sizes[0] * sizes[1]
    shells = weight.shape[1]
    vmem = pl.BlockSpec(memory_space=pltpu.VMEM)
    return pl.pallas_call(
        functools.partial(exchange_kernel, sizes, shells),
        out_shape=jax.ShapeDtypeStruct((GROUPS_DEV, shells), jnp.float32),
        in_specs=[vmem, vmem],
        out_specs=vmem,
        scratch_shapes=[
            pltpu.VMEM((n, GROUPS_DEV, parts.shape[-1]), jnp.float32),
            pltpu.SemaphoreType.DMA((n,)),
            pltpu.SemaphoreType.DMA((n,)),
        ],
        compiler_params=pltpu.CompilerParams(collective_id=1, has_side_effects=True),
        name="exchange_groups",
    )(parts.reshape(n, GROUPS_DEV, parts.shape[-1]), weight)


def body(sizes, images, slices, classes, rotations, defocus, groups):
    doms, clss = sizes
    n = doms * clss
    count, _, pixels = images.shape
    side = math.isqrt(pixels)
    classes_here, rot_count = slices.shape[:2]

    def rows_of(array):
        lead = array.shape[:-2]
        split = array.reshape(lead + (2, side, side))
        return jnp.swapaxes(split, -3, -2).reshape(lead + (2 * side, side))

    own = rows_of(slices).reshape(classes_here * rot_count, 2 * side, side)
    ny = clss // 2
    if clss % 2 == 0 and doms % ny == 0 and n <= 32:
        every = gather((ny, ny, doms // ny), own)
    else:
        every = lax.all_gather(own, AXES, axis=0)
    every = every.reshape(n * own.shape[0], 2 * side, side)
    index = classes * rot_count + rotations
    parts = shell_power(rows_of(images), every, index, defocus, groups, GROUPS_DEV * n)
    offsets = np.arange(side)
    signed = np.where(offsets < side // 2, offsets, offsets - side)
    radius = signed[:, None] ** 2 + signed[None, :] ** 2
    s = np.arange(side // 2)[:, None, None]
    weight = ((s * s <= radius) & (radius < (s + 1) ** 2)).sum(axis=(1, 2)).astype(np.float32)
    return exchange(sizes, parts, jnp.asarray(weight).reshape(1, -1))


def solution(mesh):
    sizes = (mesh.shape["dom"], mesh.shape["cls"])
    return jax.shard_map(
        functools.partial(body, sizes),
        mesh=mesh,
        in_specs=(
            P(AXES, None, None),
            P(AXES, None, None, None),
            P(AXES),
            P(AXES),
            P(AXES),
            P(AXES),
        ),
        out_specs=P(AXES, None),
        check_vma=False,
    )
```

```python
import functools
import math

import jax
import jax.numpy as jnp
import numpy as np
from jax import lax
from jax.experimental import pallas as pl
from jax.experimental.pallas import tpu as pltpu
from jax.sharding import PartitionSpec as P

GROUPS_DEV = 8
PIXEL_SIZE = 1.5
WAVELENGTH = 0.0197
SPHERICAL = 27000000.0
AMPLITUDE = 0.1
ROUND = 12582912.0
MESH = pl.DeviceIdType.MESH
AXES = ("dom", "cls")
ROUTES = (("x", "y", "z"), ("z", "y", "x"), ("z", "x", "y"))
SHARE = (8, 12, 12)


def sine_coefficients(terms):
    nodes = 0.5 * np.cos((np.arange(400) + 0.5) * math.pi / 400)
    nodes = nodes[np.abs(nodes) > 1e-3]
    basis = np.stack([nodes ** (2 * k + 1) for k in range(terms)], 1)
    return np.linalg.lstsq(basis, np.sin(2 * math.pi * nodes), rcond=None)[0]


SINE = [float(v) for v in sine_coefficients(6)]


def gather_kernel(shape, own_ref, out_ref, local_sem, send_sem, recv_sem, pair_send, pair_recv):
    size = dict(x=shape[0], y=shape[1], z=shape[2])
    dom, cls = lax.axis_index("dom"), lax.axis_index("cls")
    here = dict(x=cls // 2, y=dom % size["y"], z=dom // size["y"])
    core = cls % 2
    rows = out_ref.shape[2]
    starts = [0]
    for share in SHARE:
        starts.append(starts[-1] + rows * share // 32)

    def device(at, which):
        return (at["z"] * size["y"] + at["y"], at["x"] * 2 + which)

    def slot(at, which):
        d = device(at, which)
        return d[0] * (size["x"] * 2) + d[1]

    def moved(at, dim, step):
        new = dict(at)
        new[dim] = at[dim] + step
        return new

    ways = []
    for dim in "xyz":
        if size[dim] == 1:
            continue
        if size[dim] == 2:
            other = dict(here)
            other[dim] = 1 - here[dim]
            ways.append((dim, 0, other, None))
        else:
            ways.append((dim, 1, moved(here, dim, 1), here[dim] < size[dim] - 1))
            ways.append((dim, -1, moved(here, dim, -1), here[dim] > 0))

    def when(conds, fn):
        conds = [c for c in conds if c is not None]
        if not conds:
            fn()
        else:
            pl.when(functools.reduce(jnp.logical_and, conds))(fn)

    barrier = pltpu.get_barrier_semaphore()
    partner = device(here, 1 - core)
    pl.semaphore_signal(barrier, inc=1, device_id=partner, device_id_type=MESH)
    for dim, sign, other, ok in ways:

        def greet(other=other):
            pl.semaphore_signal(barrier, inc=1, device_id=device(other, core), device_id_type=MESH)

        when([ok], greet)
    peers = 1
    for dim, sign, other, ok in ways:
        peers = peers + (1 if ok is None else ok.astype(jnp.int32))
    pl.semaphore_wait(barrier, peers)

    mine = slot(here, core)
    local = pltpu.make_async_copy(own_ref, out_ref.at[mine], local_sem)
    local.start()

    def part(ref, index):
        return ref.at[:, pl.ds(starts[index], starts[index + 1] - starts[index]), :]

    def copy(index, source, src_slot, to, way, own):
        src = part(own_ref, index) if own else part(out_ref.at[src_slot], index)
        return pltpu.make_async_remote_copy(
            src_ref=src,
            dst_ref=part(out_ref.at[src_slot], index),
            send_sem=send_sem.at[index, source, way],
            recv_sem=recv_sem.at[index, src_slot],
            device_id=to,
            device_id_type=MESH,
        )

    def pair_copy(index, source, src_slot, own):
        src = part(own_ref, index) if own else part(out_ref.at[src_slot], index)
        return pltpu.make_async_remote_copy(
            src_ref=src,
            dst_ref=part(out_ref.at[src_slot], index),
            send_sem=pair_send.at[index, source],
            recv_sem=pair_recv.at[index, src_slot],
            device_id=partner,
            device_id_type=MESH,
        )

    choices = {}
    for dim in "xyz":
        n = size[dim]
        if n == 1:
            choices[dim] = [(0, here[dim], None, 0)]
        elif n == 2:
            choices[dim] = [(0, here[dim], None, 0), (0, 1 - here[dim], None, 1)]
        else:
            listed = [(0, here[dim], None, 0)]
            for t in range(1, n):
                listed.append((1, here[dim] - t, here[dim] >= t, t))
                listed.append((-1, here[dim] + t, here[dim] + t < n, t))
            choices[dim] = listed
    events = []
    for ix, cx in enumerate(choices["x"]):
        for iy, cy in enumerate(choices["y"]):
            for iz, cz in enumerate(choices["z"]):
                pick = dict(x=cx, y=cy, z=cz)
                depth = cx[3] + cy[3] + cz[3]
                number = (ix * len(choices["y"]) + iy) * len(choices["z"]) + iz
                for index in range(3):
                    events.append((depth, index, number, pick))
    events.sort(key=lambda e: e[:3])
    finish = []
    for depth, index, number, pick in events:
        at = {dim: pick[dim][1] for dim in "xyz"}
        exists = [pick[dim][2] for dim in "xyz"]
        src_slot = slot(at, core)
        order = ROUTES[index]
        last = max([k for k, dim in enumerate(order) if pick[dim][3] > 0], default=-1)
        sends = []
        for number_way, (dim, sign, other, ok) in enumerate(ways):
            k = order.index(dim)
            if k < last:
                continue
            if k == last and (size[dim] == 2 or sign != pick[dim][0]):
                continue
            sends.append((number_way, device(other, core), ok))

        def arrive(index=index, number=number, src_slot=src_slot, depth=depth, sends=sends):
            own = depth == 0
            if not own:
                copy(index, number, src_slot, partner, 0, False).wait_recv()
            for way, to, ok in sends:
                when([ok], copy(index, number, src_slot, to, way, own).start)
            pair_copy(index, number, src_slot, own).start()

        def done(index=index, number=number, src_slot=src_slot, depth=depth, sends=sends, at=at):
            own = depth == 0
            for way, to, ok in sends:
                when([ok], copy(index, number, src_slot, to, way, own).wait_send)
            pair_copy(index, number, src_slot, own).wait_send()
            pair_copy(index, number, slot(at, 1 - core), False).wait_recv()

        when(exists, arrive)
        finish.append((exists, done))
    for exists, done in finish:
        when(exists, done)
    local.wait()


def gather(shape, own):
    devices = 2 * shape[0] * shape[1] * shape[2]
    total = 1
    for n in shape:
        total *= n if n <= 2 else 2 * n - 1
    return pl.pallas_call(
        functools.partial(gather_kernel, shape),
        out_shape=jax.ShapeDtypeStruct((devices,) + own.shape, own.dtype),
        in_specs=[pl.BlockSpec(memory_space=pltpu.VMEM)],
        out_specs=pl.BlockSpec(memory_space=pltpu.VMEM),
        scratch_shapes=[
            pltpu.SemaphoreType.DMA,
            pltpu.SemaphoreType.DMA((3, total, 4)),
            pltpu.SemaphoreType.DMA((3, devices)),
            pltpu.SemaphoreType.DMA((3, total)),
            pltpu.SemaphoreType.DMA((3, devices)),
        ],
        compiler_params=pltpu.CompilerParams(
            collective_id=0, has_side_effects=True, vmem_limit_bytes=12 * 1024 * 1024
        ),
        name="gather_slices",
    )(own)


def power_kernel(
    side, rot_count, classes_ref, rotations_ref, defocus_ref, images_ref, slices_ref, slope_ref, offset_ref, groups_ref, out_ref, power, acc
):
    step = pl.program_id(0)
    count, chunk, lanes = images_ref.shape
    shells = side // 2
    pitch = power.shape[0] // count

    @pl.when(step == 0)
    def _():
        acc[...] = jnp.zeros_like(acc)

    slope = slope_ref[...]
    offset = offset_ref[...]

    def one(i, carry):
        turns = defocus_ref[i].astype(jnp.float32) * slope + offset
        x = turns - ((turns + ROUND) - ROUND)
        y = x * x
        s = jnp.full_like(y, SINE[-1])
        for value in SINE[-2::-1]:
            s = s * y + value
        s = s * x
        d = images_ref[i].astype(jnp.float32) + s * slices_ref[classes_ref[i] * rot_count + rotations_ref[i]].astype(jnp.float32)
        power[pl.ds(pl.multiple_of(i * pitch, 8), chunk), :] = d * d
        return carry

    lax.fori_loop(0, count, one, 0, unroll=4)

    b = lax.broadcasted_iota(jnp.int32, (lanes, shells), 0)
    s = lax.broadcasted_iota(jnp.int32, (lanes, shells), 1)
    fb = jnp.where(b < side // 2, b, b - side)
    total = acc[...]
    for k in range(chunk // 2):
        a = step * (chunk // 2) + k
        fa = jnp.where(a < side // 2, a, a - side)
        r = fa * fa + fb * fb
        table = jnp.where((s * s <= r) & (r < (s + 1) * (s + 1)), 1.0, 0.0).astype(jnp.bfloat16)
        p = power[pl.ds(2 * k, count, stride=pitch), :] + power[pl.ds(2 * k + 1, count, stride=pitch), :]
        high = p.astype(jnp.bfloat16)
        low = (p - high.astype(jnp.float32)).astype(jnp.bfloat16)
        total = total + jnp.dot(
            jnp.concatenate([high, low], axis=1),
            jnp.concatenate([table, table], axis=0),
            preferred_element_type=jnp.float32,
        )
    acc[...] = total

    @pl.when(step == pl.num_programs(0) - 1)
    def _():
        groups = out_ref.shape[0]
        ids = lax.broadcasted_iota(jnp.int32, (groups, count), 0)
        member = jnp.where(ids == groups_ref[...], 1.0, 0.0)
        both = jnp.concatenate([acc[...], jnp.ones((count, out_ref.shape[1] - shells), jnp.float32)], axis=1)
        out_ref[...] = jnp.dot(
            member, both, precision=lax.Precision.HIGHEST, preferred_element_type=jnp.float32
        )


def shell_power(images, slices, classes, rotations, rot_count, defocus, groups, group_total):
    count, rows, side = images.shape
    chunk = 32
    offsets = np.arange(side)
    signed = np.where(offsets < side // 2, offsets, offsets - side)
    radius = (signed[:, None] ** 2 + signed[None, :] ** 2).astype(np.float64)
    spatial = np.repeat(radius / (side * PIXEL_SIZE) ** 2, 2, axis=0)
    slope = (0.5 * WAVELENGTH * spatial).astype(np.float32)
    offset = -0.25 * SPHERICAL * WAVELENGTH**3 * spatial**2 + math.asin(AMPLITUDE) / (2 * math.pi)
    offset = (offset - np.round(offset)).astype(np.float32)
    smem = pl.BlockSpec(memory_space=pltpu.SMEM)
    return pl.pallas_call(
        functools.partial(power_kernel, side, rot_count),
        grid=(rows // chunk,),
        out_shape=jax.ShapeDtypeStruct((group_total, 128), jnp.float32),
        in_specs=[
            smem,
            smem,
            smem,
            pl.BlockSpec((count, chunk, side), lambda i: (0, i, 0)),
            pl.BlockSpec((slices.shape[0], chunk, side), lambda i: (0, i, 0)),
            pl.BlockSpec((chunk, side), lambda i: (i, 0)),
            pl.BlockSpec((chunk, side), lambda i: (i, 0)),
            pl.BlockSpec((1, count), lambda i: (0, 0)),
        ],
        out_specs=pl.BlockSpec((group_total, 128), lambda i: (0, 0)),
        scratch_shapes=[
            pltpu.VMEM((count * (chunk + 8), side), jnp.float32),
            pltpu.VMEM((count, side // 2), jnp.float32),
        ],
        compiler_params=pltpu.CompilerParams(vmem_limit_bytes=20 * 1024 * 1024),
        name="shell_power",
    )(classes, rotations, defocus, images, slices, jnp.asarray(slope), jnp.asarray(offset), groups.reshape(1, count))


def exchange_kernel(sizes, shells, parts_ref, weight_ref, out_ref, held, send_sem, recv_sem):
    doms, clss = sizes
    n = doms * clss
    me = lax.axis_index("dom") * clss + lax.axis_index("cls")
    barrier = pltpu.get_barrier_semaphore()

    def device(k):
        peer = lax.rem(me + k, n)
        return peer, (peer // clss, lax.rem(peer, clss))

    def greet(k, carry):
        pl.semaphore_signal(barrier, inc=1, device_id=device(k)[1], device_id_type=MESH)
        return carry

    lax.fori_loop(1, n, greet, 0)
    pl.semaphore_wait(barrier, n - 1)

    def copy(k):
        peer, to = device(k)
        return pltpu.make_async_remote_copy(
            src_ref=parts_ref.at[peer],
            dst_ref=held.at[k],
            send_sem=send_sem.at[k],
            recv_sem=recv_sem.at[k],
            device_id=to,
            device_id_type=MESH,
        )

    def send(k, carry):
        copy(k).start()
        return carry

    lax.fori_loop(1, n, send, 0)

    def take(k, total):
        copy(k).wait_recv()
        return total + held[k]

    total = lax.fori_loop(1, n, take, parts_ref[me])

    def sent(k, carry):
        copy(k).wait_send()
        return carry

    lax.fori_loop(1, n, sent, 0)
    counts = total[:, shells : shells + 1]
    out_ref[...] = total[:, :shells] / (2.0 * counts * weight_ref[...])


def exchange(sizes, parts, weight):
    n = sizes[0] * sizes[1]
    shells = weight.shape[1]
    vmem = pl.BlockSpec(memory_space=pltpu.VMEM)
    return pl.pallas_call(
        functools.partial(exchange_kernel, sizes, shells),
        out_shape=jax.ShapeDtypeStruct((GROUPS_DEV, shells), jnp.float32),
        in_specs=[vmem, vmem],
        out_specs=vmem,
        scratch_shapes=[
            pltpu.VMEM((n, GROUPS_DEV, parts.shape[-1]), jnp.float32),
            pltpu.SemaphoreType.DMA((n,)),
            pltpu.SemaphoreType.DMA((n,)),
        ],
        compiler_params=pltpu.CompilerParams(
            collective_id=1, has_side_effects=True, vmem_limit_bytes=4 * 1024 * 1024
        ),
        name="exchange_groups",
    )(parts.reshape(n, GROUPS_DEV, parts.shape[-1]), weight)


def body(sizes, images, slices, classes, rotations, defocus, groups):
    doms, clss = sizes
    n = doms * clss
    count, _, pixels = images.shape
    side = math.isqrt(pixels)
    classes_here, rot_count = slices.shape[:2]

    def rows_of(array):
        lead = array.shape[:-2]
        split = array.reshape(lead + (2, side, side))
        return jnp.swapaxes(split, -3, -2).reshape(lead + (2 * side, side))

    own = rows_of(slices).reshape(classes_here * rot_count, 2 * side, side)
    ny = clss // 2
    if clss % 2 == 0 and doms % ny == 0 and n <= 32:
        every = gather((ny, ny, doms // ny), own)
    else:
        every = lax.all_gather(own, AXES, axis=0)
    every = every.reshape(n * own.shape[0], 2 * side, side)
    parts = shell_power(rows_of(images), every, classes, rotations, rot_count, defocus, groups, GROUPS_DEV * n)
    offsets = np.arange(side)
    signed = np.where(offsets < side // 2, offsets, offsets - side)
    radius = signed[:, None] ** 2 + signed[None, :] ** 2
    s = np.arange(side // 2)[:, None, None]
    weight = ((s * s <= radius) & (radius < (s + 1) ** 2)).sum(axis=(1, 2)).astype(np.float32)
    return exchange(sizes, parts, jnp.asarray(weight).reshape(1, -1))


def solution(mesh):
    sizes = (mesh.shape["dom"], mesh.shape["cls"])
    return jax.shard_map(
        functools.partial(body, sizes),
        mesh=mesh,
        in_specs=(
            P(AXES, None, None),
            P(AXES, None, None, None),
            P(AXES),
            P(AXES),
            P(AXES),
            P(AXES),
        ),
        out_specs=P(AXES, None),
        check_vma=False,
    )
```

```python
import functools
import math

import jax
import jax.numpy as jnp
import numpy as np
from jax import lax
from jax.experimental import pallas as pl
from jax.experimental.pallas import tpu as pltpu
from jax.sharding import PartitionSpec as P

GROUPS_DEV = 8
PIXEL_SIZE = 1.5
WAVELENGTH = 0.0197
SPHERICAL = 27000000.0
AMPLITUDE = 0.1
ROUND = 12582912.0
MESH = pl.DeviceIdType.MESH
AXES = ("dom", "cls")
ROUTES = (("x", "y", "z"), ("z", "y", "x"), ("z", "x", "y"))
SHARE = (8, 12, 12)


def sine_coefficients(terms):
    nodes = 0.5 * np.cos((np.arange(400) + 0.5) * math.pi / 400)
    nodes = nodes[np.abs(nodes) > 1e-3]
    basis = np.stack([nodes ** (2 * k + 1) for k in range(terms)], 1)
    return np.linalg.lstsq(basis, np.sin(2 * math.pi * nodes), rcond=None)[0]


SINE = [float(v) for v in sine_coefficients(5)]


def gather_kernel(shape, own_ref, out_ref, local_sem, send_sem, recv_sem, pair_send, pair_recv):
    size = dict(x=shape[0], y=shape[1], z=shape[2])
    dom, cls = lax.axis_index("dom"), lax.axis_index("cls")
    here = dict(x=cls // 2, y=dom % size["y"], z=dom // size["y"])
    core = cls % 2
    rows = out_ref.shape[2]
    starts = [0]
    for share in SHARE:
        starts.append(starts[-1] + rows * share // 32)

    def device(at, which):
        return (at["z"] * size["y"] + at["y"], at["x"] * 2 + which)

    def slot(at, which):
        d = device(at, which)
        return d[0] * (size["x"] * 2) + d[1]

    def moved(at, dim, step):
        new = dict(at)
        new[dim] = at[dim] + step
        return new

    ways = []
    for dim in "xyz":
        if size[dim] == 1:
            continue
        if size[dim] == 2:
            other = dict(here)
            other[dim] = 1 - here[dim]
            ways.append((dim, 0, other, None))
        else:
            ways.append((dim, 1, moved(here, dim, 1), here[dim] < size[dim] - 1))
            ways.append((dim, -1, moved(here, dim, -1), here[dim] > 0))

    def when(conds, fn):
        conds = [c for c in conds if c is not None]
        if not conds:
            fn()
        else:
            pl.when(functools.reduce(jnp.logical_and, conds))(fn)

    barrier = pltpu.get_barrier_semaphore()
    partner = device(here, 1 - core)
    pl.semaphore_signal(barrier, inc=1, device_id=partner, device_id_type=MESH)
    for dim, sign, other, ok in ways:

        def greet(other=other):
            pl.semaphore_signal(barrier, inc=1, device_id=device(other, core), device_id_type=MESH)

        when([ok], greet)
    peers = 1
    for dim, sign, other, ok in ways:
        peers = peers + (1 if ok is None else ok.astype(jnp.int32))
    pl.semaphore_wait(barrier, peers)

    mine = slot(here, core)
    local = pltpu.make_async_copy(own_ref, out_ref.at[mine], local_sem)
    local.start()

    def part(ref, index):
        return ref.at[:, pl.ds(starts[index], starts[index + 1] - starts[index]), :]

    def copy(index, source, src_slot, to, way, own):
        src = part(own_ref, index) if own else part(out_ref.at[src_slot], index)
        return pltpu.make_async_remote_copy(
            src_ref=src,
            dst_ref=part(out_ref.at[src_slot], index),
            send_sem=send_sem.at[index, source, way],
            recv_sem=recv_sem.at[index, src_slot],
            device_id=to,
            device_id_type=MESH,
        )

    def pair_copy(index, source, src_slot, own):
        src = part(own_ref, index) if own else part(out_ref.at[src_slot], index)
        return pltpu.make_async_remote_copy(
            src_ref=src,
            dst_ref=part(out_ref.at[src_slot], index),
            send_sem=pair_send.at[index, source],
            recv_sem=pair_recv.at[index, src_slot],
            device_id=partner,
            device_id_type=MESH,
        )

    choices = {}
    for dim in "xyz":
        n = size[dim]
        if n == 1:
            choices[dim] = [(0, here[dim], None, 0)]
        elif n == 2:
            choices[dim] = [(0, here[dim], None, 0), (0, 1 - here[dim], None, 1)]
        else:
            listed = [(0, here[dim], None, 0)]
            for t in range(1, n):
                listed.append((1, here[dim] - t, here[dim] >= t, t))
                listed.append((-1, here[dim] + t, here[dim] + t < n, t))
            choices[dim] = listed
    events = []
    for ix, cx in enumerate(choices["x"]):
        for iy, cy in enumerate(choices["y"]):
            for iz, cz in enumerate(choices["z"]):
                pick = dict(x=cx, y=cy, z=cz)
                depth = cx[3] + cy[3] + cz[3]
                number = (ix * len(choices["y"]) + iy) * len(choices["z"]) + iz
                for index in range(3):
                    events.append((depth, index, number, pick))
    events.sort(key=lambda e: e[:3])
    finish = []
    for depth, index, number, pick in events:
        at = {dim: pick[dim][1] for dim in "xyz"}
        exists = [pick[dim][2] for dim in "xyz"]
        src_slot = slot(at, core)
        order = ROUTES[index]
        last = max([k for k, dim in enumerate(order) if pick[dim][3] > 0], default=-1)
        sends = []
        for number_way, (dim, sign, other, ok) in enumerate(ways):
            k = order.index(dim)
            if k < last:
                continue
            if k == last and (size[dim] == 2 or sign != pick[dim][0]):
                continue
            sends.append((number_way, device(other, core), ok))

        def arrive(index=index, number=number, src_slot=src_slot, depth=depth, sends=sends):
            own = depth == 0
            if not own:
                copy(index, number, src_slot, partner, 0, False).wait_recv()
            for way, to, ok in sends:
                when([ok], copy(index, number, src_slot, to, way, own).start)
            pair_copy(index, number, src_slot, own).start()

        def done(index=index, number=number, src_slot=src_slot, depth=depth, sends=sends, at=at):
            own = depth == 0
            for way, to, ok in sends:
                when([ok], copy(index, number, src_slot, to, way, own).wait_send)
            pair_copy(index, number, src_slot, own).wait_send()
            pair_copy(index, number, slot(at, 1 - core), False).wait_recv()

        when(exists, arrive)
        finish.append((exists, done))
    for exists, done in finish:
        when(exists, done)
    local.wait()


def gather(shape, own):
    devices = 2 * shape[0] * shape[1] * shape[2]
    total = 1
    for n in shape:
        total *= n if n <= 2 else 2 * n - 1
    return pl.pallas_call(
        functools.partial(gather_kernel, shape),
        out_shape=jax.ShapeDtypeStruct((devices,) + own.shape, own.dtype),
        in_specs=[pl.BlockSpec(memory_space=pltpu.VMEM)],
        out_specs=pl.BlockSpec(memory_space=pltpu.VMEM),
        scratch_shapes=[
            pltpu.SemaphoreType.DMA,
            pltpu.SemaphoreType.DMA((3, total, 4)),
            pltpu.SemaphoreType.DMA((3, devices)),
            pltpu.SemaphoreType.DMA((3, total)),
            pltpu.SemaphoreType.DMA((3, devices)),
        ],
        compiler_params=pltpu.CompilerParams(
            collective_id=0, has_side_effects=True, vmem_limit_bytes=12 * 1024 * 1024
        ),
        name="gather_slices",
    )(own)


def power_kernel(
    side, rot_count, classes_ref, rotations_ref, defocus_ref, images_ref, slices_ref, slope_ref, offset_ref, groups_ref, out_ref, power, acc
):
    step = pl.program_id(0)
    count, chunk, lanes = images_ref.shape
    shells = side // 2
    pitch = power.shape[0] // count

    @pl.when(step == 0)
    def _():
        acc[...] = jnp.zeros_like(acc)

    slope = slope_ref[...]
    offset = offset_ref[...]

    def one(i, carry):
        turns = defocus_ref[i].astype(jnp.float32) * slope + offset
        x = turns - ((turns + ROUND) - ROUND)
        y = x * x
        s = jnp.full_like(y, SINE[-1])
        for value in SINE[-2::-1]:
            s = s * y + value
        s = s * x
        d = images_ref[i].astype(jnp.float32) + s * slices_ref[classes_ref[i] * rot_count + rotations_ref[i]].astype(jnp.float32)
        power[pl.ds(pl.multiple_of(i * pitch, 8), chunk), :] = d * d
        return carry

    lax.fori_loop(0, count, one, 0, unroll=8)

    b = lax.broadcasted_iota(jnp.int32, (lanes, shells), 0)
    s = lax.broadcasted_iota(jnp.int32, (lanes, shells), 1)
    fb = jnp.where(b < side // 2, b, b - side)
    total = acc[...]
    for k in range(chunk // 2):
        a = step * (chunk // 2) + k
        fa = jnp.where(a < side // 2, a, a - side)
        r = fa * fa + fb * fb
        table = jnp.where((s * s <= r) & (r < (s + 1) * (s + 1)), 1.0, 0.0).astype(jnp.bfloat16)
        p = power[pl.ds(2 * k, count, stride=pitch), :] + power[pl.ds(2 * k + 1, count, stride=pitch), :]
        high = p.astype(jnp.bfloat16)
        low = (p - high.astype(jnp.float32)).astype(jnp.bfloat16)
        total = total + jnp.dot(
            jnp.concatenate([high, low], axis=1),
            jnp.concatenate([table, table], axis=0),
            preferred_element_type=jnp.float32,
        )
    acc[...] = total

    @pl.when(step == pl.num_programs(0) - 1)
    def _():
        groups = out_ref.shape[0]
        ids = lax.broadcasted_iota(jnp.int32, (groups, count), 0)
        member = jnp.where(ids == groups_ref[...], 1.0, 0.0)
        both = jnp.concatenate([acc[...], jnp.ones((count, out_ref.shape[1] - shells), jnp.float32)], axis=1)
        out_ref[...] = jnp.dot(
            member, both, precision=lax.Precision.HIGHEST, preferred_element_type=jnp.float32
        )


def shell_power(images, slices, classes, rotations, rot_count, defocus, groups, group_total):
    count, rows, side = images.shape
    chunk = 32
    offsets = np.arange(side)
    signed = np.where(offsets < side // 2, offsets, offsets - side)
    radius = (signed[:, None] ** 2 + signed[None, :] ** 2).astype(np.float64)
    spatial = np.repeat(radius / (side * PIXEL_SIZE) ** 2, 2, axis=0)
    slope = (0.5 * WAVELENGTH * spatial).astype(np.float32)
    offset = -0.25 * SPHERICAL * WAVELENGTH**3 * spatial**2 + math.asin(AMPLITUDE) / (2 * math.pi)
    offset = (offset - np.round(offset)).astype(np.float32)
    smem = pl.BlockSpec(memory_space=pltpu.SMEM)
    return pl.pallas_call(
        functools.partial(power_kernel, side, rot_count),
        grid=(rows // chunk,),
        out_shape=jax.ShapeDtypeStruct((group_total, 128), jnp.float32),
        in_specs=[
            smem,
            smem,
            smem,
            pl.BlockSpec((count, chunk, side), lambda i: (0, i, 0)),
            pl.BlockSpec((slices.shape[0], chunk, side), lambda i: (0, i, 0)),
            pl.BlockSpec((chunk, side), lambda i: (i, 0)),
            pl.BlockSpec((chunk, side), lambda i: (i, 0)),
            pl.BlockSpec((1, count), lambda i: (0, 0)),
        ],
        out_specs=pl.BlockSpec((group_total, 128), lambda i: (0, 0)),
        scratch_shapes=[
            pltpu.VMEM((count * (chunk + 8), side), jnp.float32),
            pltpu.VMEM((count, side // 2), jnp.float32),
        ],
        compiler_params=pltpu.CompilerParams(vmem_limit_bytes=20 * 1024 * 1024),
        name="shell_power",
    )(classes, rotations, defocus, images, slices, jnp.asarray(slope), jnp.asarray(offset), groups.reshape(1, count))


def exchange_kernel(sizes, shells, parts_ref, weight_ref, out_ref, held, send_sem, recv_sem):
    doms, clss = sizes
    n = doms * clss
    me = lax.axis_index("dom") * clss + lax.axis_index("cls")
    barrier = pltpu.get_barrier_semaphore()

    def device(k):
        peer = lax.rem(me + k, n)
        return peer, (peer // clss, lax.rem(peer, clss))

    def greet(k, carry):
        pl.semaphore_signal(barrier, inc=1, device_id=device(k)[1], device_id_type=MESH)
        return carry

    lax.fori_loop(1, n, greet, 0)
    pl.semaphore_wait(barrier, n - 1)

    def copy(k):
        peer, to = device(k)
        return pltpu.make_async_remote_copy(
            src_ref=parts_ref.at[peer],
            dst_ref=held.at[k],
            send_sem=send_sem.at[k],
            recv_sem=recv_sem.at[k],
            device_id=to,
            device_id_type=MESH,
        )

    def send(k, carry):
        copy(k).start()
        return carry

    lax.fori_loop(1, n, send, 0)

    def take(k, total):
        copy(k).wait_recv()
        return total + held[k]

    total = lax.fori_loop(1, n, take, parts_ref[me])

    def sent(k, carry):
        copy(k).wait_send()
        return carry

    lax.fori_loop(1, n, sent, 0)
    counts = total[:, shells : shells + 1]
    out_ref[...] = total[:, :shells] / (2.0 * counts * weight_ref[...])


def exchange(sizes, parts, weight):
    n = sizes[0] * sizes[1]
    shells = weight.shape[1]
    vmem = pl.BlockSpec(memory_space=pltpu.VMEM)
    return pl.pallas_call(
        functools.partial(exchange_kernel, sizes, shells),
        out_shape=jax.ShapeDtypeStruct((GROUPS_DEV, shells), jnp.float32),
        in_specs=[vmem, vmem],
        out_specs=vmem,
        scratch_shapes=[
            pltpu.VMEM((n, GROUPS_DEV, parts.shape[-1]), jnp.float32),
            pltpu.SemaphoreType.DMA((n,)),
            pltpu.SemaphoreType.DMA((n,)),
        ],
        compiler_params=pltpu.CompilerParams(
            collective_id=1, has_side_effects=True, vmem_limit_bytes=4 * 1024 * 1024
        ),
        name="exchange_groups",
    )(parts.reshape(n, GROUPS_DEV, parts.shape[-1]), weight)


def body(sizes, images, slices, classes, rotations, defocus, groups):
    doms, clss = sizes
    n = doms * clss
    count, _, pixels = images.shape
    side = math.isqrt(pixels)
    classes_here, rot_count = slices.shape[:2]

    def rows_of(array):
        lead = array.shape[:-2]
        split = array.reshape(lead + (2, side, side))
        return jnp.swapaxes(split, -3, -2).reshape(lead + (2 * side, side))

    own = rows_of(slices).reshape(classes_here * rot_count, 2 * side, side)
    ny = clss // 2
    if clss % 2 == 0 and doms % ny == 0 and n <= 32:
        every = gather((ny, ny, doms // ny), own)
    else:
        every = lax.all_gather(own, AXES, axis=0)
    every = every.reshape(n * own.shape[0], 2 * side, side)
    parts = shell_power(rows_of(images), every, classes, rotations, rot_count, defocus, groups, GROUPS_DEV * n)
    offsets = np.arange(side)
    signed = np.where(offsets < side // 2, offsets, offsets - side)
    radius = signed[:, None] ** 2 + signed[None, :] ** 2
    s = np.arange(side // 2)[:, None, None]
    weight = ((s * s <= radius) & (radius < (s + 1) ** 2)).sum(axis=(1, 2)).astype(np.float32)
    return exchange(sizes, parts, jnp.asarray(weight).reshape(1, -1))


def solution(mesh):
    sizes = (mesh.shape["dom"], mesh.shape["cls"])
    return jax.shard_map(
        functools.partial(body, sizes),
        mesh=mesh,
        in_specs=(
            P(AXES, None, None),
            P(AXES, None, None, None),
            P(AXES),
            P(AXES),
            P(AXES),
            P(AXES),
        ),
        out_specs=P(AXES, None),
        check_vma=False,
    )
```
